32 devices in a mesh: rep: 8 (over z, x), tp: 4 (over y, core).
Axes of the slice: x: 2, y: 2, z: 4, core: 2. Of those that a mesh axis runs over, the one named last changes fastest.
Arguments:
- stream_in: bfloat16 [32, 4, 8192], P('rep', None, 'tp'), may hold values from -6 to 6
- queries: bfloat16 [32, 4, 4096], P('rep'), may hold values from -90 to 90
- new_keys: bfloat16 [32, 4, 4, 128], P('rep'), may hold values from -4 to 4
- new_values: bfloat16 [32, 4, 4, 128], P('rep'), may hold values from -4 to 4
- key_cache: bfloat16 [32, 1024, 4, 128], P('rep', 'tp'), may hold values from -4.1 to 4.1
- value_cache: bfloat16 [32, 1024, 4, 128], P('rep', 'tp'), may hold values from -4 to 4
- lengths: int32 [32], P('rep'), may hold values from 2 to 1024
- out_weight: bfloat16 [4096, 8192], P('tp', 'rep'), may hold values from -0.09375 to 0.09375
- norm_gain: bfloat16 [8192], P('tp'), may hold values from 0.5 to 1.5
Outputs:
- stream_out: bfloat16 [32, 4, 8192], P('rep', None, 'tp')
- normed: bfloat16 [32, 4, 8192], P('rep', None, 'tp')
The draws below stay inside these ranges and needn't reach their ends.
All inputs are finite; a program needn't handle non-finite values.
Results may differ from the reference program's by a relative error of at most 0.0065.
Values may be sent and summed in bfloat16 or wider, within the bound.
A program may use at most 64 MiB of HBM per device.

```python
import math
import jax
import jax.numpy as jnp
from jax import lax

D = 8192
HEADS = 32
KV_HEADS = 4
HD = 128
STEPS = 4
ROWS = 32
CTX = 1024
FEAT = 4096
N_TP = 4


def shared_keys(key):
    base = jax.random.normal(jax.random.fold_in(key, 11), (ROWS, CTX, KV_HEADS, HD), jnp.float32)
    base = jnp.clip(base, -4.0, 4.0)
    return base


def draw_key_cache(key, part):
    return shared_keys(key).astype(jnp.bfloat16)


def draw_queries(key, part):
    drawn = jax.random.normal(jax.random.fold_in(key, 23), (ROWS, STEPS, HEADS * HD), jnp.float32)
    drawn = jnp.clip(drawn, -4.0, 4.0)
    return drawn.astype(jnp.bfloat16)


def plant(values, stream_key, least, top_value):
    longest = values.shape.index(max(values.shape))
    spots = []
    for shift in (0, 1):
        where = [jax.random.randint(jax.random.fold_in(stream_key, axis), (), 0, length) for axis, length in enumerate(values.shape)]
        where[longest] = (where[longest] + shift) % values.shape[longest]
        spots.append(tuple(where))
    return values.at[spots[0]].set(least).at[spots[1]].set(top_value)


def levels(own_key, dims, cuts, low, largest):
    loudness = 1.0
    for position, parts in cuts:
        heights = jax.random.uniform(jax.random.fold_in(jax.random.fold_in(own_key, 6), position), (parts,), jnp.float32, low / len(cuts), largest / len(cuts))
        loudness = loudness * jnp.repeat(jnp.exp(heights), dims[position] // parts).reshape((-1,) + (1,) * (len(dims) - 1 - position))
    return loudness


def centred(own_key, extent, width, bound, shards=(), kind=jnp.bfloat16):
    result = jax.random.normal(own_key, extent, jnp.float32) * width
    if len(shards) > 0:
        result = levels(own_key, extent, shards, -0.22, 0.18) * result
    return jnp.clip(result, min=-bound, max=bound).astype(kind)


def setup_inputs(seed: int = 0) -> dict:
    key_list = jax.random.split(jax.random.key(seed), 10)
    return {
        "stream_in": centred(key_list[0], (ROWS, STEPS, D), 1.0, 6.0, ((0, 8), (2, 4))),
        "queries": draw_queries(jax.random.fold_in(key_list[9], 71), 0),
        "new_keys": centred(key_list[2], (ROWS, STEPS, KV_HEADS, HD), 1.0, 4.0, ((0, 8),)),
        "new_values": centred(key_list[3], (ROWS, STEPS, KV_HEADS, HD), 1.0, 4.0, ((0, 8),)),
        "key_cache": draw_key_cache(jax.random.fold_in(key_list[9], 71), 0),
        "value_cache": centred(key_list[5], (ROWS, CTX, KV_HEADS, HD), 1.0, 4.0, ((0, 8), (1, 4))),
        "lengths": plant(jax.random.randint(key_list[6], (ROWS,), 2, CTX + 1), jax.random.fold_in(key_list[6], 1), 2, CTX).astype(jnp.int32),
        "out_weight": centred(key_list[7], (FEAT, D), FEAT ** -0.5, 0.09375, ((0, 4), (1, 8))),
        "norm_gain": jnp.clip(1.0 + 0.1 * jax.random.normal(key_list[8], (D,), jnp.float32), 0.5, 1.5).astype(jnp.bfloat16),
    }


def attend_row(packed):
    query, key_new, value_new, key_old, value_old, length = packed
    group_size = HEADS // KV_HEADS
    scaling = 1.0 / math.sqrt(HD)
    query_f = query.astype(jnp.float32).reshape(STEPS, KV_HEADS, group_size, HD)
    cached = jnp.einsum('sgjd,pgd->sgjp', query_f, key_old.astype(jnp.float32)) * scaling
    visible = jnp.arange(CTX) < length
    cached = jnp.where(visible[None, None, None, :], cached, -1e+30)
    fresh = jnp.einsum('sgjd,tgd->sgjt', query_f, key_new.astype(jnp.float32)) * scaling
    causal = jnp.arange(STEPS)[None, :] <= jnp.arange(STEPS)[:, None]
    fresh = jnp.where(causal[:, None, None, :], fresh, -1e+30)
    maxima = jnp.maximum(cached.max(-1), fresh.max(-1))
    weights_cached = jnp.exp(cached - maxima[..., None])
    weights_fresh = jnp.exp(fresh - maxima[..., None])
    denominator = weights_cached.sum(-1) + weights_fresh.sum(-1)
    rounded_cached = lax.optimization_barrier(weights_cached.astype(jnp.bfloat16)).astype(jnp.float32)
    rounded_fresh = lax.optimization_barrier(weights_fresh.astype(jnp.bfloat16)).astype(jnp.float32)
    numerator = jnp.einsum('sgjp,pgd->sgjd', rounded_cached, value_old.astype(jnp.float32))
    numerator = numerator + jnp.einsum('sgjt,tgd->sgjd', rounded_fresh, value_new.astype(jnp.float32))
    attended = (numerator / denominator[..., None]).astype(jnp.bfloat16)
    return attended.reshape(STEPS, HEADS * HD)

def reference(stream_in, queries, new_keys, new_values, key_cache, value_cache, lengths, out_weight, norm_gain):
    attended = lax.map(attend_row, (queries, new_keys, new_values, key_cache, value_cache, lengths))
    flat = attended.reshape(ROWS * STEPS, HEADS * HD)
    width_share = HEADS * HD // N_TP
    summed = jnp.zeros((ROWS * STEPS, D), jnp.float32)
    for group_index in range(N_TP):
        lower = group_index * width_share
        partial_value = jnp.dot(flat[:, lower:lower + width_share], out_weight[lower:lower + width_share], preferred_element_type=jnp.float32)
        summed = summed + lax.optimization_barrier(partial_value.astype(jnp.bfloat16)).astype(jnp.float32)
    hidden = stream_in.reshape(ROWS * STEPS, D).astype(jnp.float32) + summed
    inverse = lax.rsqrt(lax.optimization_barrier(jnp.mean(hidden * hidden, axis=1)) + 1e-06)
    normed = hidden * inverse[:, None] * norm_gain.astype(jnp.float32)[None, :]
    stream_out = hidden.astype(jnp.bfloat16).reshape(ROWS, STEPS, D)
    return (stream_out, normed.astype(jnp.bfloat16).reshape(ROWS, STEPS, D))
```

```python
import functools
import math

import jax
import jax.numpy as jnp
from jax import lax
from jax.experimental import pallas as pl
from jax.experimental.pallas import tpu as pltpu
from jax.sharding import PartitionSpec as P

MESH = pl.DeviceIdType.MESH
PAD = 128


def kernel(
    cfg,
    lengths_ref,
    q_hbm, nk_hbm, nv_hbm, k_hbm, v_hbm, w_hbm, x_hbm, gain_hbm,
    stream_ref, normed_ref,
    q_v, k_v, v_v, w_v, x_v, gain_v,
    send_o, recv_o, send_l, recv_l,
    gathered, parts, recv_p, sq_send, sq_recv,
    load_sem, kv_sem,
    ao_send, ao_recv, al_send, al_recv, b_send, b_recv, c_send, c_recv, d_send, d_recv,
):
    n_rep, n_tp, batch, steps, heads, kv, block_len, width_all, eps = cfg
    rep = lax.axis_index("rep")
    tp = lax.axis_index("tp")
    k_own = n_rep // n_tp
    rows = batch * steps
    owned = heads // n_tp
    orow = owned * steps
    cached = block_len * kv
    fresh = steps * kv
    cw = parts.shape[2]
    hd = q_v.shape[2]
    owner = rep // k_own
    is_own = owner == tp

    loads = [pltpu.make_async_copy(q_hbm, q_v, load_sem.at[0])]
    loads[0].start()
    kv_loads = []
    for b in range(batch):
        group = [
            pltpu.make_async_copy(k_hbm.at[b], k_v.at[b, pl.ds(0, cached)], kv_sem.at[b, 0]),
            pltpu.make_async_copy(nk_hbm.at[b], k_v.at[b, pl.ds(cached, fresh)], kv_sem.at[b, 1]),
            pltpu.make_async_copy(v_hbm.at[b], v_v.at[b, pl.ds(0, cached)], kv_sem.at[b, 2]),
            pltpu.make_async_copy(nv_hbm.at[b], v_v.at[b, pl.ds(cached, fresh)], kv_sem.at[b, 3]),
        ]
        for c in group:
            c.start()
        kv_loads.append(group)
    late = [
        pltpu.make_async_copy(w_hbm, w_v, load_sem.at[1]),
        pltpu.make_async_copy(x_hbm, x_v, load_sem.at[2]),
        pltpu.make_async_copy(gain_hbm, gain_v, load_sem.at[3]),
    ]
    for c in late:
        c.start()

    barrier = pltpu.get_barrier_semaphore()
    for j in range(1, n_tp):
        pl.semaphore_signal(barrier, inc=1, device_id=(rep, lax.rem(tp + j, n_tp)), device_id_type=MESH)
    for j in range(1, n_rep):
        pl.semaphore_signal(barrier, inc=1, device_id=(lax.rem(rep + j, n_rep), tp), device_id_type=MESH)
    for i in range(k_own):
        for t in range(n_tp):
            src_rep = tp * k_own + i

            @pl.when(jnp.logical_not((src_rep == rep) & (tp == t)))
            def _():
                pl.semaphore_signal(barrier, inc=1, device_id=(src_rep, t), device_id_type=MESH)

    for b in range(batch):
        pad = jnp.zeros((PAD - fresh, hd), jnp.bfloat16)
        k_v[b, cached + fresh : cached + PAD, :] = pad
        v_v[b, cached + fresh : cached + PAD, :] = pad

    hs = heads * steps
    cols = cached + PAD
    scaling = 1.0 / math.sqrt(hd)
    row_i = lax.broadcasted_iota(jnp.int32, (hs, cols), 0)
    col_i = lax.broadcasted_iota(jnp.int32, (hs, cols), 1)
    same = (row_i // (steps * (heads // kv))) == (col_i % kv)
    is_cached = col_i < cached
    new_t = (col_i - cached) // kv
    causal = (new_t <= row_i % steps) & (col_i < cached + fresh) & (tp == 0)
    keep = same & (is_cached | causal)
    far = jnp.int32(2**30)
    position = jnp.where(keep, jnp.where(is_cached, tp * block_len + col_i // kv, -1), far)
    lane = lax.broadcasted_iota(jnp.int32, (hs, 128), 1)
    lse = jnp.zeros((hs, 128), jnp.float32)
    loads[0].wait()
    for b in range(batch):
        for c in kv_loads[b]:
            c.wait()
        s = lax.dot_general(
            q_v[b], k_v[b], (((1,), (1,)), ((), ())), preferred_element_type=jnp.float32
        )
        s = jnp.where(position < lengths_ref[b], s * scaling, -1e30)
        top = jnp.max(s, axis=1, keepdims=True)
        p = jnp.exp(s - top)
        total = jnp.sum(p, axis=1, keepdims=True)
        num = jnp.dot(p.astype(jnp.bfloat16), v_v[b], preferred_element_type=jnp.float32)
        out = (num / total).astype(jnp.bfloat16)
        for t in range(n_tp):
            send_o[t, b] = out[t * orow : (t + 1) * orow]
        lse = jnp.where(lane == b, top + jnp.log(total), lse)
    for t in range(n_tp):
        send_l[t] = lse[t * orow : (t + 1) * orow]

    arrivals = (n_tp - 1) + (n_rep - 1) + n_rep - is_own.astype(jnp.int32)
    pl.semaphore_wait(barrier, arrivals)

    sends = []
    for j in range(1, n_tp):
        peer = lax.rem(tp + j, n_tp)
        c1 = pltpu.make_async_remote_copy(
            send_l.at[peer], recv_l.at[tp], al_send.at[j], al_recv.at[tp],
            device_id=(rep, peer), device_id_type=MESH)
        c1.start()
        c2 = pltpu.make_async_remote_copy(
            send_o.at[peer], recv_o.at[tp], ao_send.at[j], ao_recv.at[tp],
            device_id=(rep, peer), device_id_type=MESH)
        c2.start()
        sends += [c1, c2]
    for j in range(1, n_tp):
        peer = lax.rem(tp + j, n_tp)
        pltpu.make_async_remote_copy(
            send_l.at[peer], recv_l.at[peer], al_send.at[j], al_recv.at[peer],
            device_id=(rep, peer), device_id_type=MESH).wait_recv()
        pltpu.make_async_remote_copy(
            send_o.at[peer], recv_o.at[peer], ao_send.at[j], ao_recv.at[peer],
            device_id=(rep, peer), device_id_type=MESH).wait_recv()
    ls = [send_l[tp]] + [recv_l[lax.rem(tp + j, n_tp)] for j in range(1, n_tp)]
    os_ = [send_o[tp]] + [recv_o[lax.rem(tp + j, n_tp)] for j in range(1, n_tp)]
    most = functools.reduce(jnp.maximum, ls)
    ws = [jnp.exp(l - most) for l in ls]
    inv = 1.0 / functools.reduce(jnp.add, ws)
    ws = [w * inv for w in ws]
    att = []
    for b in range(batch):
        acc = ws[0][:, b : b + 1] * os_[0][b].astype(jnp.float32)
        for t in range(1, n_tp):
            acc = acc + ws[t][:, b : b + 1] * os_[t][b].astype(jnp.float32)
        att.append(acc.astype(jnp.bfloat16))
    att = jnp.concatenate(att, axis=0)
    m = batch * orow
    to = lax.broadcasted_iota(jnp.int32, (m, m), 0)
    frm = lax.broadcasted_iota(jnp.int32, (m, m), 1)
    want = ((to // steps) % batch) * orow + (to // rows) * steps + to % steps
    pick = jnp.where(frm == want, 1.0, 0.0).astype(jnp.bfloat16)
    att = jnp.dot(pick, att, preferred_element_type=jnp.float32).astype(jnp.bfloat16)
    gathered[rep] = jnp.concatenate([att[h * rows : (h + 1) * rows] for h in range(owned)], axis=1)

    for j in range(1, n_rep):
        peer = lax.rem(rep + j, n_rep)
        c = pltpu.make_async_remote_copy(
            gathered.at[rep], gathered.at[rep], b_send.at[j], b_recv.at[rep],
            device_id=(peer, tp), device_id_type=MESH)
        c.start()
        sends.append(c)
    late[0].wait()
    for j in range(1, n_rep):
        peer = lax.rem(rep + j, n_rep)
        pltpu.make_async_remote_copy(
            gathered.at[peer], gathered.at[peer], b_send.at[j], b_recv.at[peer],
            device_id=(peer, tp), device_id_type=MESH).wait_recv()
    full = gathered[...].reshape(n_rep * rows, gathered.shape[2])
    proj = jnp.dot(full, w_v[...], preferred_element_type=jnp.float32).astype(jnp.bfloat16)
    parts[...] = proj.reshape(n_rep, rows, cw)

    slot = lax.rem(rep, k_own) * n_tp + tp
    for j in range(1, n_rep):
        peer = lax.rem(rep + j, n_rep)
        c = pltpu.make_async_remote_copy(
            parts.at[peer], recv_p.at[slot], c_send.at[j], c_recv.at[slot],
            device_id=(peer, owner), device_id_type=MESH)
        c.start()
        sends.append(c)
    mine = pltpu.make_async_remote_copy(
        parts.at[rep], recv_p.at[slot], c_send.at[0], c_recv.at[slot],
        device_id=(rep, owner), device_id_type=MESH)

    @pl.when(is_own)
    def _():
        recv_p[slot] = parts[rep]

    @pl.when(jnp.logical_not(is_own))
    def _():
        mine.start()

    late[1].wait()
    late[2].wait()
    for i in range(k_own):
        for t in range(n_tp):
            sid = i * n_tp + t
            src_rep = tp * k_own + i

            @pl.when(jnp.logical_not((src_rep == rep) & (tp == t)))
            def _():
                pltpu.make_async_remote_copy(
                    parts.at[0], recv_p.at[sid], c_send.at[0], c_recv.at[sid],
                    device_id=(src_rep, t), device_id_type=MESH).wait_recv()

    pieces = []
    for i in range(k_own):
        acc = recv_p[i * n_tp].astype(jnp.float32)
        for t in range(1, n_tp):
            acc = acc + recv_p[i * n_tp + t].astype(jnp.float32)
        pieces.append(acc)
    summed = jnp.concatenate(pieces, axis=1)
    x = x_v[...].astype(jnp.float32).reshape(rows, x_v.shape[2])
    hidden = x + summed
    squares = jnp.sum(hidden * hidden, axis=1, keepdims=True)

    sq_send[...] = jnp.broadcast_to(squares, sq_send.shape)
    for j in range(1, n_tp):
        peer = lax.rem(tp + j, n_tp)
        c = pltpu.make_async_remote_copy(
            sq_send, sq_recv.at[tp], d_send.at[j], d_recv.at[tp],
            device_id=(rep, peer), device_id_type=MESH)
        c.start()
        sends.append(c)
    stream_ref[...] = hidden.astype(jnp.bfloat16).reshape(stream_ref.shape)
    gained = hidden * gain_v[...].astype(jnp.float32)
    every = sq_send[...]
    for j in range(1, n_tp):
        peer = lax.rem(tp + j, n_tp)
        pltpu.make_async_remote_copy(
            sq_send, sq_recv.at[peer], d_send.at[j], d_recv.at[peer],
            device_id=(rep, peer), device_id_type=MESH).wait_recv()
        every = every + sq_recv[peer]
    inverse = lax.rsqrt(every[:, :1] / width_all + eps)
    normed_ref[...] = (gained * inverse).astype(jnp.bfloat16).reshape(normed_ref.shape)

    for c in sends:
        c.wait_send()

    @pl.when(jnp.logical_not(is_own))
    def _():
        mine.wait_send()


def on_device(
    n_rep, n_tp,
    stream_in, queries, new_keys, new_values, key_cache, value_cache, lengths, out_weight, norm_gain
):
    batch, steps, width = queries.shape
    block_len, kv, hd = key_cache.shape[1:]
    heads = width // hd
    depth, cw = out_weight.shape
    own_w = stream_in.shape[2]
    rows = batch * steps
    assert n_rep % n_tp == 0 and heads % n_tp == 0
    owned = heads // n_tp
    orow = owned * steps
    hs = heads * steps
    cached = block_len * kv
    q = queries.reshape(batch, steps, heads, hd).transpose(0, 2, 1, 3).reshape(batch, hs, hd)
    nk = new_keys.reshape(batch, steps * kv, hd)
    nv = new_values.reshape(batch, steps * kv, hd)
    kc = key_cache.reshape(batch, cached, hd)
    vc = value_cache.reshape(batch, cached, hd)
    cfg = (n_rep, n_tp, batch, steps, heads, kv, block_len, own_w * n_tp, 1e-6)
    bf, f32 = jnp.bfloat16, jnp.float32
    anyspec = pl.BlockSpec(memory_space=pl.ANY)
    dma = pltpu.SemaphoreType.DMA
    return pl.pallas_call(
        functools.partial(kernel, cfg),
        out_shape=(
            jax.ShapeDtypeStruct(stream_in.shape, bf),
            jax.ShapeDtypeStruct(stream_in.shape, bf),
        ),
        in_specs=[pl.BlockSpec(memory_space=pltpu.SMEM)] + [anyspec] * 8,
        out_specs=(pl.BlockSpec(memory_space=pltpu.VMEM), pl.BlockSpec(memory_space=pltpu.VMEM)),
        scratch_shapes=[
            pltpu.VMEM((batch, hs, hd), bf),
            pltpu.VMEM((batch, cached + PAD, hd), bf),
            pltpu.VMEM((batch, cached + PAD, hd), bf),
            pltpu.VMEM((depth, cw), bf),
            pltpu.VMEM((batch, steps, own_w), bf),
            pltpu.VMEM((1, own_w), bf),
            pltpu.VMEM((n_tp, batch, orow, hd), bf),
            pltpu.VMEM((n_tp, batch, orow, hd), bf),
            pltpu.VMEM((n_tp, orow, 128), f32),
            pltpu.VMEM((n_tp, orow, 128), f32),
            pltpu.VMEM((n_rep, rows, depth), bf),
            pltpu.VMEM((n_rep, rows, cw), bf),
            pltpu.VMEM((n_rep, rows, cw), bf),
            pltpu.VMEM((rows, 128), f32),
            pltpu.VMEM((n_tp, rows, 128), f32),
            dma((4,)),
            dma((batch, 4)),
            dma((n_tp,)), dma((n_tp,)), dma((n_tp,)), dma((n_tp,)),
            dma((n_rep,)), dma((n_rep,)), dma((n_rep,)), dma((n_rep,)),
            dma((n_tp,)), dma((n_tp,)),
        ],
        compiler_params=pltpu.CompilerParams(collective_id=0, has_side_effects=True),
    )(lengths, q, nk, nv, kc, vc, out_weight, stream_in, norm_gain.reshape(1, own_w))


def solution(mesh):
    return jax.shard_map(
        functools.partial(on_device, mesh.shape["rep"], mesh.shape["tp"]),
        mesh=mesh,
        in_specs=(
            P("rep", None, "tp"),
            P("rep", None, None),
            P("rep", None, None, None),
            P("rep", None, None, None),
            P("rep", "tp", None, None),
            P("rep", "tp", None, None),
            P("rep"),
            P("tp", "rep"),
            P("tp"),
        ),
        out_specs=(P("rep", None, "tp"), P("rep", None, "tp")),
        check_vma=False,
    )
```

```python
import functools
import math

import jax
import jax.numpy as jnp
from jax import lax
from jax.experimental import pallas as pl
from jax.experimental.pallas import tpu as pltpu
from jax.sharding import PartitionSpec as P

MESH = pl.DeviceIdType.MESH
PAD = 128


def flip(index, mask, count):
    other = 0
    bit = 1
    while bit < count:
        digit = (index // bit) % 2
        other = other + bit * ((1 - digit) if mask & bit else digit)
        bit *= 2
    return other


def kernel(
    cfg,
    lengths_ref,
    q_hbm, nk_hbm, nv_hbm, k_hbm, v_hbm, w_hbm, x_hbm, gain_hbm,
    stream_ref, normed_ref,
    q_v, k_v, v_v, w_v, x_v, gain_v,
    send_o, recv_o, send_l, recv_l,
    gathered, parts, recv_p, sq_send, sq_recv,
    load_sem, kv_sem,
    ao_send, ao_recv, al_send, al_recv, b_send, b_recv, c_send, c_recv, d_send, d_recv,
):
    n_rep, n_tp, batch, steps, heads, kv, block_len, width_all, eps = cfg
    rep = lax.axis_index("rep")
    tp = lax.axis_index("tp")
    k_own = n_rep // n_tp
    rows = batch * steps
    owned = heads // n_tp
    orow = owned * steps
    cached = block_len * kv
    fresh = steps * kv
    cw = parts.shape[2]
    hd = q_v.shape[2]
    owner = rep // k_own
    is_own = owner == tp

    sends = []
    half = batch // 2 if batch % 2 == 0 else batch
    parts_a = batch // half
    barrier = pltpu.get_barrier_semaphore()
    for j in range(1, n_tp):
        pl.semaphore_signal(barrier, inc=1, device_id=(rep, lax.rem(tp + j, n_tp)), device_id_type=MESH)
    for j in range(1, n_rep):
        pl.semaphore_signal(barrier, inc=1, device_id=(lax.rem(rep + j, n_rep), tp), device_id_type=MESH)
    for i in range(k_own):
        for t in range(n_tp):
            src_rep = tp * k_own + i

            @pl.when(jnp.logical_not((src_rep == rep) & (tp == t)))
            def _():
                pl.semaphore_signal(barrier, inc=1, device_id=(src_rep, t), device_id_type=MESH)

    loads = [pltpu.make_async_copy(q_hbm, q_v, load_sem.at[0])]
    loads[0].start()
    kv_loads = []
    for b in range(batch):
        group = [
            pltpu.make_async_copy(k_hbm.at[b], k_v.at[b, pl.ds(0, cached)], kv_sem.at[b, 0]),
            pltpu.make_async_copy(nk_hbm.at[b], k_v.at[b, pl.ds(cached, fresh)], kv_sem.at[b, 1]),
            pltpu.make_async_copy(v_hbm.at[b], v_v.at[b, pl.ds(0, cached)], kv_sem.at[b, 2]),
            pltpu.make_async_copy(nv_hbm.at[b], v_v.at[b, pl.ds(cached, fresh)], kv_sem.at[b, 3]),
        ]
        for c in group:
            c.start()
        kv_loads.append(group)
    late = [
        pltpu.make_async_copy(w_hbm, w_v, load_sem.at[1]),
        pltpu.make_async_copy(x_hbm, x_v, load_sem.at[2]),
        pltpu.make_async_copy(gain_hbm, gain_v, load_sem.at[3]),
    ]
    for c in late:
        c.start()

    for b in range(batch):
        pad = jnp.zeros((PAD - fresh, hd), jnp.bfloat16)
        k_v[b, cached + fresh : cached + PAD, :] = pad
        v_v[b, cached + fresh : cached + PAD, :] = pad

    hs = heads * steps
    cols = cached + PAD
    scaling = 1.0 / math.sqrt(hd)
    row_i = lax.broadcasted_iota(jnp.int32, (hs, cols), 0)
    col_i = lax.broadcasted_iota(jnp.int32, (hs, cols), 1)
    same = (row_i // (steps * (heads // kv))) == (col_i % kv)
    is_cached = col_i < cached
    new_t = (col_i - cached) // kv
    causal = (new_t <= row_i % steps) & (col_i < cached + fresh) & (tp == 0)
    keep = same & (is_cached | causal)
    far = jnp.int32(2**30)
    position = jnp.where(keep, jnp.where(is_cached, tp * block_len + col_i // kv, -1), far)
    lane = lax.broadcasted_iota(jnp.int32, (hs, 128), 1)
    lse = jnp.zeros((hs, 128), jnp.float32)
    loads[0].wait()
    for b in range(batch):
        for c in kv_loads[b]:
            c.wait()
        s = lax.dot_general(
            q_v[b], k_v[b], (((1,), (1,)), ((), ())), preferred_element_type=jnp.float32
        )
        s = jnp.where(position < lengths_ref[b], s * scaling, -1e30)
        top = jnp.max(s, axis=1, keepdims=True)
        p = jnp.exp(s - top)
        total = jnp.sum(p, axis=1, keepdims=True)
        num = jnp.dot(p.astype(jnp.bfloat16), v_v[b], preferred_element_type=jnp.float32)
        out = (num / total).astype(jnp.bfloat16)
        for t in range(n_tp):
            send_o[t, b] = out[t * orow : (t + 1) * orow]
        lse = jnp.where(lane == b, top + jnp.log(total), lse)
        if (b + 1) % half == 0:
            part = b // half
            if part == 0:
                arrivals = (n_tp - 1) + (n_rep - 1) + n_rep - is_own.astype(jnp.int32)
                pl.semaphore_wait(barrier, arrivals)
            if part == parts_a - 1:
                for t in range(n_tp):
                    send_l[t] = lse[t * orow : (t + 1) * orow]
            span = pl.ds(part * half, half)
            for j in range(1, n_tp):
                peer = lax.rem(tp + j, n_tp)
                if part == parts_a - 1:
                    c = pltpu.make_async_remote_copy(
                        send_l.at[peer], recv_l.at[tp], al_send.at[j], al_recv.at[tp],
                        device_id=(rep, peer), device_id_type=MESH)
                    c.start()
                    sends.append(c)
                c = pltpu.make_async_remote_copy(
                    send_o.at[peer, span], recv_o.at[tp, span], ao_send.at[part, j], ao_recv.at[part, tp],
                    device_id=(rep, peer), device_id_type=MESH)
                c.start()
                sends.append(c)

    for j in range(1, n_tp):
        peer = lax.rem(tp + j, n_tp)
        pltpu.make_async_remote_copy(
            send_l.at[peer], recv_l.at[peer], al_send.at[j], al_recv.at[peer],
            device_id=(rep, peer), device_id_type=MESH).wait_recv()
        for part in range(parts_a):
            span = pl.ds(part * half, half)
            pltpu.make_async_remote_copy(
                send_o.at[peer, span], recv_o.at[peer, span], ao_send.at[part, j], ao_recv.at[part, peer],
                device_id=(rep, peer), device_id_type=MESH).wait_recv()
    ls = [send_l[tp]] + [recv_l[lax.rem(tp + j, n_tp)] for j in range(1, n_tp)]
    os_ = [send_o[tp]] + [recv_o[lax.rem(tp + j, n_tp)] for j in range(1, n_tp)]
    most = functools.reduce(jnp.maximum, ls)
    ws = [jnp.exp(l - most) for l in ls]
    inv = 1.0 / functools.reduce(jnp.add, ws)
    ws = [w * inv for w in ws]
    att = []
    for b in range(batch):
        acc = ws[0][:, b : b + 1] * os_[0][b].astype(jnp.float32)
        for t in range(1, n_tp):
            acc = acc + ws[t][:, b : b + 1] * os_[t][b].astype(jnp.float32)
        att.append(acc.astype(jnp.bfloat16))
    att = jnp.concatenate(att, axis=0)
    m = batch * orow
    to = lax.broadcasted_iota(jnp.int32, (m, m), 0)
    frm = lax.broadcasted_iota(jnp.int32, (m, m), 1)
    want = ((to // steps) % batch) * orow + (to // rows) * steps + to % steps
    pick = jnp.where(frm == want, 1.0, 0.0).astype(jnp.bfloat16)
    att = jnp.dot(pick, att, preferred_element_type=jnp.float32).astype(jnp.bfloat16)
    gathered[rep] = jnp.concatenate([att[h * rows : (h + 1) * rows] for h in range(owned)], axis=1)

    for mask in range(n_rep - 1, 0, -1):
        peer = flip(rep, mask, n_rep)
        c = pltpu.make_async_remote_copy(
            gathered.at[rep], gathered.at[rep], b_send.at[mask], b_recv.at[rep],
            device_id=(peer, tp), device_id_type=MESH)
        c.start()
        sends.append(c)
    late[0].wait()
    slot = lax.rem(rep, k_own) * n_tp + tp
    mine = pltpu.make_async_remote_copy(
        parts.at[rep], recv_p.at[slot], c_send.at[0], c_recv.at[slot],
        device_id=(rep, owner), device_id_type=MESH)
    for pair in range(n_rep // 2 - 1, -1, -1):
        masks = (2 * pair + 1, 2 * pair)
        peers = [flip(rep, mask, n_rep) for mask in masks]
        for mask, peer in zip(masks, peers):
            if mask:
                pltpu.make_async_remote_copy(
                    gathered.at[peer], gathered.at[peer], b_send.at[mask], b_recv.at[peer],
                    device_id=(peer, tp), device_id_type=MESH).wait_recv()
        block = jnp.concatenate([gathered[peer] for peer in peers], axis=0)
        proj = jnp.dot(block, w_v[...], preferred_element_type=jnp.float32).astype(jnp.bfloat16)
        for i, (mask, peer) in enumerate(zip(masks, peers)):
            parts[peer] = proj[i * rows : (i + 1) * rows]
            if mask:
                c = pltpu.make_async_remote_copy(
                    parts.at[peer], recv_p.at[slot], c_send.at[mask], c_recv.at[slot],
                    device_id=(peer, owner), device_id_type=MESH)
                c.start()
                sends.append(c)

    @pl.when(is_own)
    def _():
        recv_p[slot] = parts[rep]

    @pl.when(jnp.logical_not(is_own))
    def _():
        mine.start()

    late[1].wait()
    late[2].wait()
    gain = gain_v[...].astype(jnp.float32)
    gain = jnp.concatenate([gain[c : c + 1] for c in range(gain.shape[0])], axis=1)
    x = x_v[...].astype(jnp.float32).reshape(rows, x_v.shape[2])
    for i in range(k_own):
        for t in range(n_tp):
            sid = i * n_tp + t
            src_rep = tp * k_own + i

            @pl.when(jnp.logical_not((src_rep == rep) & (tp == t)))
            def _():
                pltpu.make_async_remote_copy(
                    parts.at[0], recv_p.at[sid], c_send.at[0], c_recv.at[sid],
                    device_id=(src_rep, t), device_id_type=MESH).wait_recv()

    pieces = []
    for i in range(k_own):
        acc = recv_p[i * n_tp].astype(jnp.float32)
        for t in range(1, n_tp):
            acc = acc + recv_p[i * n_tp + t].astype(jnp.float32)
        pieces.append(acc)
    summed = jnp.concatenate(pieces, axis=1)
    hidden = x + summed
    squares = jnp.sum(hidden * hidden, axis=1, keepdims=True)

    sq_send[...] = jnp.broadcast_to(squares, sq_send.shape)
    for j in range(1, n_tp):
        peer = lax.rem(tp + j, n_tp)
        c = pltpu.make_async_remote_copy(
            sq_send, sq_recv.at[tp], d_send.at[j], d_recv.at[tp],
            device_id=(rep, peer), device_id_type=MESH)
        c.start()
        sends.append(c)
    stream_ref[...] = hidden.astype(jnp.bfloat16).reshape(stream_ref.shape)
    gained = hidden * gain
    every = sq_send[...]
    for j in range(1, n_tp):
        peer = lax.rem(tp + j, n_tp)
        pltpu.make_async_remote_copy(
            sq_send, sq_recv.at[peer], d_send.at[j], d_recv.at[peer],
            device_id=(rep, peer), device_id_type=MESH).wait_recv()
        every = every + sq_recv[peer]
    inverse = lax.rsqrt(every[:, :1] / width_all + eps)
    normed_ref[...] = (gained * inverse).astype(jnp.bfloat16).reshape(normed_ref.shape)

    for c in sends:
        c.wait_send()

    @pl.when(jnp.logical_not(is_own))
    def _():
        mine.wait_send()


def on_device(
    n_rep, n_tp,
    stream_in, queries, new_keys, new_values, key_cache, value_cache, lengths, out_weight, norm_gain
):
    batch, steps, width = queries.shape
    block_len, kv, hd = key_cache.shape[1:]
    heads = width // hd
    depth, cw = out_weight.shape
    own_w = stream_in.shape[2]
    rows = batch * steps
    assert n_rep & (n_rep - 1) == 0
    assert n_rep % n_tp == 0 and heads % n_tp == 0
    owned = heads // n_tp
    orow = owned * steps
    hs = heads * steps
    cached = block_len * kv
    q = queries.reshape(batch, steps, heads, hd).transpose(0, 2, 1, 3).reshape(batch, hs, hd)
    nk = new_keys.reshape(batch, steps * kv, hd)
    nv = new_values.reshape(batch, steps * kv, hd)
    kc = key_cache.reshape(batch, cached, hd)
    vc = value_cache.reshape(batch, cached, hd)
    cfg = (n_rep, n_tp, batch, steps, heads, kv, block_len, own_w * n_tp, 1e-6)
    bf, f32 = jnp.bfloat16, jnp.float32
    anyspec = pl.BlockSpec(memory_space=pl.ANY)
    dma = pltpu.SemaphoreType.DMA
    return pl.pallas_call(
        functools.partial(kernel, cfg),
        out_shape=(
            pltpu.VMEM(stream_in.shape, bf),
            pltpu.VMEM(stream_in.shape, bf),
        ),
        in_specs=[pl.BlockSpec(memory_space=pltpu.SMEM)] + [anyspec] * 8,
        out_specs=(pl.BlockSpec(memory_space=pltpu.VMEM), pl.BlockSpec(memory_space=pltpu.VMEM)),
        scratch_shapes=[
            pltpu.VMEM((batch, hs, hd), bf),
            pltpu.VMEM((batch, cached + PAD, hd), bf),
            pltpu.VMEM((batch, cached + PAD, hd), bf),
            pltpu.VMEM((depth, cw), bf),
            pltpu.VMEM((batch, steps, own_w), bf),
            pltpu.VMEM((own_w // 128, 128), bf),
            pltpu.VMEM((n_tp, batch, orow, hd), bf),
            pltpu.VMEM((n_tp, batch, orow, hd), bf),
            pltpu.VMEM((n_tp, orow, 128), f32),
            pltpu.VMEM((n_tp, orow, 128), f32),
            pltpu.VMEM((n_rep, rows, depth), bf),
            pltpu.VMEM((n_rep, rows, cw), bf),
            pltpu.VMEM((n_rep, rows, cw), bf),
            pltpu.VMEM((rows, 128), f32),
            pltpu.VMEM((n_tp, rows, 128), f32),
            dma((4,)),
            dma((batch, 4)),
            dma((batch, n_tp)), dma((batch, n_tp)), dma((n_tp,)), dma((n_tp,)),
            dma((n_rep,)), dma((n_rep,)), dma((n_rep,)), dma((n_rep,)),
            dma((n_tp,)), dma((n_tp,)),
        ],
        compiler_params=pltpu.CompilerParams(collective_id=0, has_side_effects=True),
    )(lengths, q, nk, nv, kc, vc, out_weight, stream_in, norm_gain.reshape(own_w // 128, 128))


def solution(mesh):
    return jax.shard_map(
        functools.partial(on_device, mesh.shape["rep"], mesh.shape["tp"]),
        mesh=mesh,
        in_specs=(
            P("rep", None, "tp"),
            P("rep", None, None),
            P("rep", None, None, None),
            P("rep", None, None, None),
            P("rep", "tp", None, None),
            P("rep", "tp", None, None),
            P("rep"),
            P("tp", "rep"),
            P("tp"),
        ),
        out_specs=(P("rep", None, "tp"), P("rep", None, "tp")),
        check_vma=False,
    )
```

```python
import functools
import math

import jax
import jax.numpy as jnp
from jax import lax
from jax.experimental import pallas as pl
from jax.experimental.pallas import tpu as pltpu
from jax.sharding import PartitionSpec as P

MESH = pl.DeviceIdType.MESH
PAD = 128


def flip(index, mask, count):
    other = 0
    bit = 1
    while bit < count:
        digit = (index // bit) % 2
        other = other + bit * ((1 - digit) if mask & bit else digit)
        bit *= 2
    return other


def kernel(
    cfg,
    lengths_ref,
    q_hbm, nk_hbm, nv_hbm, k_hbm, v_hbm, w_hbm, x_hbm, gain_hbm,
    hidden_ref, scale_ref,
    q_v, k_v, v_v, w_v, x_v, gain_v,
    send_o, recv_o, send_l, recv_l,
    gathered, parts, recv_p, sq_send, sq_recv,
    load_sem, kv_sem,
    ao_send, ao_recv, al_send, al_recv, b_send, b_recv, c_send, c_recv, d_send, d_recv,
):
    n_rep, n_tp, batch, steps, heads, kv, block_len, width_all, eps = cfg
    rep = lax.axis_index("rep")
    tp = lax.axis_index("tp")
    k_own = n_rep // n_tp
    rows = batch * steps
    owned = heads // n_tp
    orow = owned * steps
    cached = block_len * kv
    fresh = steps * kv
    cw = parts.shape[2]
    hd = q_v.shape[2]
    owner = rep // k_own
    is_own = owner == tp

    sends = []
    half = batch // 2 if batch % 2 == 0 else batch
    parts_a = batch // half
    barrier = pltpu.get_barrier_semaphore()
    for j in range(1, n_tp):
        pl.semaphore_signal(barrier, inc=1, device_id=(rep, lax.rem(tp + j, n_tp)), device_id_type=MESH)
    for j in range(1, n_rep):
        pl.semaphore_signal(barrier, inc=1, device_id=(lax.rem(rep + j, n_rep), tp), device_id_type=MESH)
    for i in range(k_own):
        for t in range(n_tp):
            src_rep = tp * k_own + i

            @pl.when(jnp.logical_not((src_rep == rep) & (tp == t)))
            def _():
                pl.semaphore_signal(barrier, inc=1, device_id=(src_rep, t), device_id_type=MESH)

    loads = [pltpu.make_async_copy(q_hbm, q_v, load_sem.at[0])]
    loads[0].start()
    kv_loads = []
    for b in range(batch):
        group = [
            pltpu.make_async_copy(k_hbm.at[b], k_v.at[b, pl.ds(0, cached)], kv_sem.at[b, 0]),
            pltpu.make_async_copy(nk_hbm.at[b], k_v.at[b, pl.ds(cached, fresh)], kv_sem.at[b, 1]),
            pltpu.make_async_copy(v_hbm.at[b], v_v.at[b, pl.ds(0, cached)], kv_sem.at[b, 2]),
            pltpu.make_async_copy(nv_hbm.at[b], v_v.at[b, pl.ds(cached, fresh)], kv_sem.at[b, 3]),
        ]
        for c in group:
            c.start()
        kv_loads.append(group)
    late = [
        pltpu.make_async_copy(w_hbm, w_v, load_sem.at[1]),
        pltpu.make_async_copy(x_hbm, x_v, load_sem.at[2]),
        pltpu.make_async_copy(gain_hbm, gain_v, load_sem.at[3]),
    ]
    for c in late:
        c.start()

    for b in range(batch):
        pad = jnp.zeros((PAD - fresh, hd), jnp.bfloat16)
        k_v[b, cached + fresh : cached + PAD, :] = pad
        v_v[b, cached + fresh : cached + PAD, :] = pad

    hs = heads * steps
    cols = cached + PAD
    scaling = 1.0 / math.sqrt(hd)
    row_i = lax.broadcasted_iota(jnp.int32, (hs, cols), 0)
    col_i = lax.broadcasted_iota(jnp.int32, (hs, cols), 1)
    same = (row_i // (steps * (heads // kv))) == (col_i % kv)
    is_cached = col_i < cached
    new_t = (col_i - cached) // kv
    causal = (new_t <= row_i % steps) & (col_i < cached + fresh) & (tp == 0)
    keep = same & (is_cached | causal)
    far = jnp.int32(2**30)
    position = jnp.where(keep, jnp.where(is_cached, tp * block_len + col_i // kv, -1), far)
    lane = lax.broadcasted_iota(jnp.int32, (hs, 128), 1)
    lse = jnp.zeros((hs, 128), jnp.float32)
    loads[0].wait()
    for b in range(batch):
        for c in kv_loads[b]:
            c.wait()
        s = lax.dot_general(
            q_v[b], k_v[b], (((1,), (1,)), ((), ())), preferred_element_type=jnp.float32
        )
        s = jnp.where(position < lengths_ref[b], s * scaling, -1e30)
        top = jnp.max(s, axis=1, keepdims=True)
        p = jnp.exp(s - top)
        total = jnp.sum(p, axis=1, keepdims=True)
        num = jnp.dot(p.astype(jnp.bfloat16), v_v[b], preferred_element_type=jnp.float32)
        out = (num / total).astype(jnp.bfloat16)
        for t in range(n_tp):
            send_o[t, b] = out[t * orow : (t + 1) * orow]
        lse = jnp.where(lane == b, top + jnp.log(total), lse)
        if (b + 1) % half == 0:
            part = b // half
            if part == 0:
                arrivals = (n_tp - 1) + (n_rep - 1) + n_rep - is_own.astype(jnp.int32)
                pl.semaphore_wait(barrier, arrivals)
            if part == parts_a - 1:
                for t in range(n_tp):
                    send_l[t] = lse[t * orow : (t + 1) * orow]
            span = pl.ds(part * half, half)
            for j in range(1, n_tp):
                peer = lax.rem(tp + j, n_tp)
                if part == parts_a - 1:
                    c = pltpu.make_async_remote_copy(
                        send_l.at[peer], recv_l.at[tp], al_send.at[j], al_recv.at[tp],
                        device_id=(rep, peer), device_id_type=MESH)
                    c.start()
                    sends.append(c)
                c = pltpu.make_async_remote_copy(
                    send_o.at[peer, span], recv_o.at[tp, span], ao_send.at[part, j], ao_recv.at[part, tp],
                    device_id=(rep, peer), device_id_type=MESH)
                c.start()
                sends.append(c)

    for j in range(1, n_tp):
        peer = lax.rem(tp + j, n_tp)
        pltpu.make_async_remote_copy(
            send_l.at[peer], recv_l.at[peer], al_send.at[j], al_recv.at[peer],
            device_id=(rep, peer), device_id_type=MESH).wait_recv()
        for part in range(parts_a):
            span = pl.ds(part * half, half)
            pltpu.make_async_remote_copy(
                send_o.at[peer, span], recv_o.at[peer, span], ao_send.at[part, j], ao_recv.at[part, peer],
                device_id=(rep, peer), device_id_type=MESH).wait_recv()
    ls = [send_l[tp]] + [recv_l[lax.rem(tp + j, n_tp)] for j in range(1, n_tp)]
    os_ = [send_o[tp]] + [recv_o[lax.rem(tp + j, n_tp)] for j in range(1, n_tp)]
    most = functools.reduce(jnp.maximum, ls)
    ws = [jnp.exp(l - most) for l in ls]
    inv = 1.0 / functools.reduce(jnp.add, ws)
    ws = [w * inv for w in ws]
    att = []
    for b in range(batch):
        acc = ws[0][:, b : b + 1] * os_[0][b].astype(jnp.float32)
        for t in range(1, n_tp):
            acc = acc + ws[t][:, b : b + 1] * os_[t][b].astype(jnp.float32)
        att.append(acc.astype(jnp.bfloat16))
    att = jnp.concatenate(att, axis=0)
    m = batch * orow
    to = lax.broadcasted_iota(jnp.int32, (m, m), 0)
    frm = lax.broadcasted_iota(jnp.int32, (m, m), 1)
    want = ((to // steps) % batch) * orow + (to // rows) * steps + to % steps
    pick = jnp.where(frm == want, 1.0, 0.0).astype(jnp.bfloat16)
    att = jnp.dot(pick, att, preferred_element_type=jnp.float32).astype(jnp.bfloat16)
    gathered[rep] = jnp.concatenate([att[h * rows : (h + 1) * rows] for h in range(owned)], axis=1)

    pairs = n_rep // 2
    mid = pairs // 2
    order = [mid, *range(mid - 1, 0, -1), *range(pairs - 1, mid, -1), 0] if mid else [0]
    for mask in [m for pair in order for m in (2 * pair + 1, 2 * pair) if m]:
        peer = flip(rep, mask, n_rep)
        c = pltpu.make_async_remote_copy(
            gathered.at[rep], gathered.at[rep], b_send.at[mask], b_recv.at[rep],
            device_id=(peer, tp), device_id_type=MESH)
        c.start()
        sends.append(c)
    late[0].wait()
    slot = lax.rem(rep, k_own) * n_tp + tp
    mine = pltpu.make_async_remote_copy(
        parts.at[rep], recv_p.at[slot], c_send.at[0], c_recv.at[slot],
        device_id=(rep, owner), device_id_type=MESH)
    for pair in order:
        masks = (2 * pair + 1, 2 * pair)
        peers = [flip(rep, mask, n_rep) for mask in masks]
        for mask, peer in zip(masks, peers):
            if mask:
                pltpu.make_async_remote_copy(
                    gathered.at[peer], gathered.at[peer], b_send.at[mask], b_recv.at[peer],
                    device_id=(peer, tp), device_id_type=MESH).wait_recv()
        block = jnp.concatenate([gathered[peer] for peer in peers], axis=0)
        proj = jnp.dot(block, w_v[...], preferred_element_type=jnp.float32).astype(jnp.bfloat16)
        for i, (mask, peer) in enumerate(zip(masks, peers)):
            parts[peer] = proj[i * rows : (i + 1) * rows]
            if mask:
                c = pltpu.make_async_remote_copy(
                    parts.at[peer], recv_p.at[slot], c_send.at[mask], c_recv.at[slot],
                    device_id=(peer, owner), device_id_type=MESH)
                c.start()
                sends.append(c)

    @pl.when(is_own)
    def _():
        recv_p[slot] = parts[rep]

    @pl.when(jnp.logical_not(is_own))
    def _():
        mine.start()

    late[1].wait()
    late[2].wait()
    gain = gain_v[...].astype(jnp.float32)
    gain = jnp.concatenate([gain[c : c + 1] for c in range(gain.shape[0])], axis=1)
    x = x_v[...].astype(jnp.float32).reshape(rows, x_v.shape[2])
    for i in range(k_own):
        for t in range(n_tp):
            sid = i * n_tp + t
            src_rep = tp * k_own + i

            @pl.when(jnp.logical_not((src_rep == rep) & (tp == t)))
            def _():
                pltpu.make_async_remote_copy(
                    parts.at[0], recv_p.at[sid], c_send.at[0], c_recv.at[sid],
                    device_id=(src_rep, t), device_id_type=MESH).wait_recv()

    pieces = []
    for i in range(k_own):
        acc = recv_p[i * n_tp].astype(jnp.float32)
        for t in range(1, n_tp):
            acc = acc + recv_p[i * n_tp + t].astype(jnp.float32)
        pieces.append(acc)
    summed = jnp.concatenate(pieces, axis=1)
    hidden = x + summed
    squares = jnp.sum(hidden * hidden, axis=1, keepdims=True)

    sq_send[...] = jnp.broadcast_to(squares, sq_send.shape)
    for j in range(1, n_tp):
        peer = lax.rem(tp + j, n_tp)
        c = pltpu.make_async_remote_copy(
            sq_send, sq_recv.at[tp], d_send.at[j], d_recv.at[tp],
            device_id=(rep, peer), device_id_type=MESH)
        c.start()
        sends.append(c)
    hidden_ref[...] = hidden.reshape(hidden_ref.shape)
    every = sq_send[...]
    for j in range(1, n_tp):
        peer = lax.rem(tp + j, n_tp)
        pltpu.make_async_remote_copy(
            sq_send, sq_recv.at[peer], d_send.at[j], d_recv.at[peer],
            device_id=(rep, peer), device_id_type=MESH).wait_recv()
        every = every + sq_recv[peer]
    inverse = lax.rsqrt(every[:, :1] / width_all + eps)
    scale_ref[...] = (inverse * gain).reshape(scale_ref.shape)

    for c in sends:
        c.wait_send()

    @pl.when(jnp.logical_not(is_own))
    def _():
        mine.wait_send()


def on_device(
    n_rep, n_tp,
    stream_in, queries, new_keys, new_values, key_cache, value_cache, lengths, out_weight, norm_gain
):
    batch, steps, width = queries.shape
    block_len, kv, hd = key_cache.shape[1:]
    heads = width // hd
    depth, cw = out_weight.shape
    own_w = stream_in.shape[2]
    rows = batch * steps
    assert n_rep & (n_rep - 1) == 0
    assert n_rep % n_tp == 0 and heads % n_tp == 0
    owned = heads // n_tp
    orow = owned * steps
    hs = heads * steps
    cached = block_len * kv
    q = queries.reshape(batch, steps, heads, hd).transpose(0, 2, 1, 3).reshape(batch, hs, hd)
    nk = new_keys.reshape(batch, steps * kv, hd)
    nv = new_values.reshape(batch, steps * kv, hd)
    kc = key_cache.reshape(batch, cached, hd)
    vc = value_cache.reshape(batch, cached, hd)
    cfg = (n_rep, n_tp, batch, steps, heads, kv, block_len, own_w * n_tp, 1e-6)
    bf, f32 = jnp.bfloat16, jnp.float32
    anyspec = pl.BlockSpec(memory_space=pl.ANY)
    dma = pltpu.SemaphoreType.DMA
    hidden, scale = pl.pallas_call(
        functools.partial(kernel, cfg),
        out_shape=(
            pltpu.VMEM(stream_in.shape, f32),
            pltpu.VMEM(stream_in.shape, f32),
        ),
        in_specs=[pl.BlockSpec(memory_space=pltpu.SMEM)] + [anyspec] * 8,
        out_specs=(pl.BlockSpec(memory_space=pltpu.VMEM), pl.BlockSpec(memory_space=pltpu.VMEM)),
        scratch_shapes=[
            pltpu.VMEM((batch, hs, hd), bf),
            pltpu.VMEM((batch, cached + PAD, hd), bf),
            pltpu.VMEM((batch, cached + PAD, hd), bf),
            pltpu.VMEM((depth, cw), bf),
            pltpu.VMEM((batch, steps, own_w), bf),
            pltpu.VMEM((own_w // 128, 128), bf),
            pltpu.VMEM((n_tp, batch, orow, hd), bf),
            pltpu.VMEM((n_tp, batch, orow, hd), bf),
            pltpu.VMEM((n_tp, orow, 128), f32),
            pltpu.VMEM((n_tp, orow, 128), f32),
            pltpu.VMEM((n_rep, rows, depth), bf),
            pltpu.VMEM((n_rep, rows, cw), bf),
            pltpu.VMEM((n_rep, rows, cw), bf),
            pltpu.VMEM((rows, 128), f32),
            pltpu.VMEM((n_tp, rows, 128), f32),
            dma((4,)),
            dma((batch, 4)),
            dma((batch, n_tp)), dma((batch, n_tp)), dma((n_tp,)), dma((n_tp,)),
            dma((n_rep,)), dma((n_rep,)), dma((n_rep,)), dma((n_rep,)),
            dma((n_tp,)), dma((n_tp,)),
        ],
        compiler_params=pltpu.CompilerParams(collective_id=0, has_side_effects=True),
    )(lengths, q, nk, nv, kc, vc, out_weight, stream_in, norm_gain.reshape(own_w // 128, 128))
    return (hidden.astype(bf), (hidden * scale).astype(bf))


def solution(mesh):
    return jax.shard_map(
        functools.partial(on_device, mesh.shape["rep"], mesh.shape["tp"]),
        mesh=mesh,
        in_specs=(
            P("rep", None, "tp"),
            P("rep", None, None),
            P("rep", None, None, None),
            P("rep", None, None, None),
            P("rep", "tp", None, None),
            P("rep", "tp", None, None),
            P("rep"),
            P("tp", "rep"),
            P("tp"),
        ),
        out_specs=(P("rep", None, "tp"), P("rep", None, "tp")),
        check_vma=False,
    )
```
